32 devices in a mesh: groups: 2 (over y), ffn: 4 (over z), hidden: 4 (over x, core).
Axes of the slice: x: 2, y: 2, z: 4, core: 2. Of those that a mesh axis runs over, the one named last changes fastest.
Arguments:
- residual_in: bfloat16 [512, 8192], P(('groups', 'ffn'), 'hidden'), parts along dimension 0, may hold values from -10 to 10
- queries: bfloat16 [512, 8192], P(('groups', 'hidden'), 'ffn'), parts along dimension 0, may hold values from -100 to 100
- new_keys: bfloat16 [512, 1024], P(('groups', 'hidden'), 'ffn'), parts along dimension 0, may hold values from -6 to 6
- new_values: bfloat16 [512, 1024], P(('groups', 'hidden'), 'ffn'), parts along dimension 0, may hold values from -24 to 24
- key_cache: bfloat16 [32, 2048, 1024], P(('groups', 'hidden'), 'ffn'), parts along dimension 0, may hold values from -6 to 6
- value_cache: bfloat16 [32, 2048, 1024], P(('groups', 'hidden'), 'ffn'), parts along dimension 0, may hold values from -24 to 24
- cache_lengths: int32 [32], P(('groups', 'hidden')), parts along dimension 0, may hold values from 1 to 2048, as said below
- norm_gain: bfloat16 [8192], P('hidden'), may hold values from 0.099609375 to 1.8984375
- out_weight: bfloat16 [8192, 8192], P('ffn', 'hidden'), may hold values from -0.25 to 0.25
- gate_weight: bfloat16 [8192, 14336], P('hidden', 'ffn'), may hold values from -0.125 to 0.125
- up_weight: bfloat16 [8192, 14336], P('hidden', 'ffn'), may hold values from -0.125 to 0.125
- down_weight: bfloat16 [14336, 8192], P('ffn', 'hidden'), may hold values from -0.09375 to 0.09375
Outputs:
- block_out: bfloat16 [512, 8192], P(('groups', 'ffn'), 'hidden'), parts along dimension 0
The draws below stay inside these ranges and needn't reach their ends.
There are 2 independent parts, one for each index of `groups`. The reference program is written for one: setup_inputs(seed, part) draws one part's arguments, and reference() takes and returns one part's arrays. A program takes and returns all parts, laid end to end along the dimension named above; an argument that names none is the same for every part. Nothing has to cross between parts.
Inputs may be any that keep to these rules, and one draw needn't show every extreme that they name: `cache_lengths`: each sequence's cached tokens fill the first cache positions; some sequence has exactly 2048.
All inputs are finite; a program needn't handle non-finite values.
Results may differ from the reference program's by a relative error of at most 0.04.
Values may be sent and summed in bfloat16 or wider, within the bound.
No kernel may reach another device: no remote copies, remote signals or barrier semaphores. Data moves between devices by JAX's collectives and lax.ppermute only.
A program may use at most 128 MiB of HBM per device.

```python
import math
import jax
import jax.numpy as jnp
from jax import lax

D = 8192
HEADS = 64
KVH = 8
HD = 128
FF = 14336
DRAFT = 16
CTX = 2048
SEQS = 16
ROWS = 256
N_FFN = 4
N_HIDDEN = 4


def draw_residual_in(key, part):
    ramp = 0.6 + 1.4 * jnp.arange(D).astype(jnp.float32) / D
    base = jnp.clip(jax.random.normal(key, (ROWS, D), jnp.float32), -5.0, 5.0)
    return (base * ramp[None, :]).astype(jnp.bfloat16)


def draw_queries(key, part):
    base = jnp.clip(jax.random.normal(key, (ROWS, HEADS * HD), jnp.float32), -4.0, 4.0)
    return base.astype(jnp.bfloat16)


def draw_cache_lengths(key, part):
    first_key, second_key = jax.random.split(jax.random.fold_in(key, 3))
    drawn = jax.random.randint(first_key, (SEQS,), 1, CTX + 1)
    chosen_seq = jax.random.randint(second_key, (), 0, SEQS)
    return jnp.where(jnp.arange(SEQS) == chosen_seq, CTX, drawn).astype(jnp.int32)


def level_of(key, extent, cuts, least, top_value):
    def one(dim, blocks):
        draws = jax.random.uniform(jax.random.fold_in(jax.random.fold_in(key, 6), dim), (blocks,), jnp.float32, least / len(cuts), top_value / len(cuts))
        return jnp.repeat(jnp.exp(draws), extent[dim] // blocks).reshape((-1,) + (1,) * (len(extent) - dim - 1))

    gain = one(*cuts[0])
    for cut in cuts[1:]:
        gain = gain * one(*cut)
    return gain


def gaussian(own_key, extent, deviation, limit, shards=(), kind=jnp.bfloat16):
    entries = jax.random.normal(own_key, extent, jnp.float32) * deviation
    if len(shards) > 0:
        entries = level_of(own_key, extent, shards, -0.22, 0.18) * entries
    return jnp.clip(entries, min=-limit, max=limit).astype(kind)


def setup_inputs(seed: int = 0, part: int = 0) -> dict:
    key_of = jax.random.split(jax.random.key(seed), 13)
    part_splits = jax.random.split(jax.random.fold_in(key_of[12], part), 13)
    return {
        "residual_in": draw_residual_in(jax.random.fold_in(jax.random.fold_in(key_of[12], part), 71), part),
        "queries": draw_queries(jax.random.fold_in(jax.random.fold_in(key_of[12], part), 71), part),
        "new_keys": gaussian(part_splits[2], (ROWS, KVH * HD), 1.0, 6.0, ((0, 4), (1, 4))),
        "new_values": gaussian(part_splits[3], (ROWS, KVH * HD), 4.0, 24.0, ((0, 4), (1, 4))),
        "key_cache": gaussian(part_splits[4], (SEQS, CTX, KVH * HD), 1.0, 6.0, ((0, 4), (1, 4))),
        "value_cache": gaussian(part_splits[5], (SEQS, CTX, KVH * HD), 4.0, 24.0, ((0, 4), (1, 4))),
        "cache_lengths": draw_cache_lengths(jax.random.fold_in(jax.random.fold_in(key_of[12], part), 71), part),
        "norm_gain": jnp.clip(1.0 + 0.18 * jax.random.normal(key_of[7], (D,), jnp.float32), 0.099609375, 1.8984375).astype(jnp.bfloat16),
        "out_weight": gaussian(key_of[8], (HEADS * HD, D), (HEADS * HD // 16) ** -0.5, 0.25, ((0, 4), (1, 4))),
        "gate_weight": gaussian(key_of[9], (D, FF), (D // 4) ** -0.5, 0.125, ((0, 4), (1, 4))),
        "up_weight": gaussian(key_of[10], (D, FF), (D // 4) ** -0.5, 0.125, ((0, 4), (1, 4))),
        "down_weight": gaussian(key_of[11], (FF, D), (FF // 4) ** -0.5, 0.09375, ((0, 4), (1, 4))),
    }


def rope_tables(positions):
    steps_half = jnp.arange(HD // 2).astype(jnp.float32)
    inverse = jnp.exp(steps_half * (-2.0 * math.log(500000.0) / HD))
    angle = positions.astype(jnp.float32)[:, None] * inverse[None, :]
    return (jnp.cos(angle), jnp.sin(angle))

def rotate(values, cosine, sine_table):
    half = values.shape[-1] // 2
    first_half = values[..., :half]
    second_half = values[..., half:]
    cosine = cosine[:, None, :]
    sine_table = sine_table[:, None, :]
    return jnp.concatenate([first_half * cosine - second_half * sine_table, second_half * cosine + first_half * sine_table], axis=-1)

def rounded(values):
    return lax.optimization_barrier(values.astype(jnp.bfloat16)).astype(jnp.float32)

def one_sequence(inputs):
    queries, new_keys, new_values, key_cache, value_cache, length = inputs
    group = HEADS // KVH
    block = CTX // N_FFN
    positions = length + jnp.arange(DRAFT, dtype=jnp.int32)
    cosine, sine_table = rope_tables(positions)
    query_rot = rounded(rotate(queries.astype(jnp.float32).reshape(DRAFT, HEADS, HD), cosine, sine_table))
    query_rot = query_rot.reshape(DRAFT, KVH, group, HD)
    key_rot = rounded(rotate(new_keys.astype(jnp.float32).reshape(DRAFT, KVH, HD), cosine, sine_table))
    cached_keys = key_cache.astype(jnp.float32).reshape(CTX, KVH, HD)
    scaling = 1.0 / math.sqrt(HD)
    cache_scores = jnp.einsum('jkgd,pkd->jkgp', query_rot, cached_keys) * scaling
    draft_scores = jnp.einsum('jkgd,ikd->jkgi', query_rot, key_rot) * scaling
    usable = jnp.arange(CTX) < length
    causal = (jnp.arange(DRAFT)[None, :] <= jnp.arange(DRAFT)[:, None])[:, None, None, :]
    cache_scores = jnp.where(usable, cache_scores, -1e+30)
    draft_scores = jnp.where(causal, draft_scores, -1e+30)
    peak_score = jnp.maximum(cache_scores.max(-1), draft_scores.max(-1))[..., None]
    cache_weights = jnp.where(usable, jnp.exp(cache_scores - peak_score), 0.0)
    draft_weights = jnp.where(causal, jnp.exp(draft_scores - peak_score), 0.0)
    cached_values = value_cache.astype(jnp.float32).reshape(N_FFN, block, KVH, HD)
    block_weights = cache_weights.reshape(DRAFT, KVH, group, N_FFN, block)
    numerator = jnp.einsum('jkgbp,bpkd->bjkgd', rounded(block_weights), cached_values)
    denominator = jnp.moveaxis(block_weights.sum(-1), -1, 0)
    draft_values = new_values.astype(jnp.float32).reshape(DRAFT, KVH, HD)
    numerator = numerator.at[0].add(jnp.einsum('jkgi,ikd->jkgd', rounded(draft_weights), draft_values))
    denominator = denominator.at[0].add(draft_weights.sum(-1))
    numerator = lax.optimization_barrier(jnp.sum(rounded(numerator), axis=0))
    denominator = lax.optimization_barrier(jnp.sum(rounded(denominator), axis=0))
    return (numerator / denominator[..., None]).reshape(DRAFT, HEADS * HD).astype(jnp.bfloat16)

def blockwise(left, right, pieces):
    width = left.shape[1] // pieces

    def add_piece(counter, total):
        offset = (counter * width).astype(jnp.int32)
        left_part = lax.dynamic_slice_in_dim(left, offset, width, 1)
        right_part = lax.dynamic_slice_in_dim(right, offset, width, 0)
        return total + rounded(jnp.dot(left_part, right_part, preferred_element_type=jnp.float32))
    initial = jnp.zeros((left.shape[0], right.shape[1]), jnp.float32)
    return lax.fori_loop(0, pieces, add_piece, initial)

def reference(residual_in, queries, new_keys, new_values, key_cache, value_cache, cache_lengths, norm_gain, out_weight, gate_weight, up_weight, down_weight):
    attended = lax.map(one_sequence, (queries.reshape(SEQS, DRAFT, HEADS * HD), new_keys.reshape(SEQS, DRAFT, KVH * HD), new_values.reshape(SEQS, DRAFT, KVH * HD), key_cache, value_cache, cache_lengths))
    attended = attended.reshape(ROWS, HEADS * HD)
    projected = blockwise(attended, out_weight, N_FFN)
    resid = (residual_in.astype(jnp.float32) + projected).astype(jnp.bfloat16)
    widened = resid.astype(jnp.float32)
    factor = lax.rsqrt(lax.optimization_barrier(jnp.mean(widened * widened, axis=1, keepdims=True)) + 1e-05)
    normed = (widened * factor * norm_gain.astype(jnp.float32)[None, :]).astype(jnp.bfloat16)
    gate = blockwise(normed, gate_weight, N_HIDDEN)
    upward = blockwise(normed, up_weight, N_HIDDEN)
    activation = (jax.nn.silu(gate) * upward).astype(jnp.bfloat16)
    lowered = blockwise(activation, down_weight, N_FFN)
    return (widened + lowered).astype(jnp.bfloat16)
```

```python
import functools
import math

import jax
import jax.numpy as jnp
from jax import lax
from jax.experimental import pallas as pl
from jax.experimental.pallas import tpu as pltpu
from jax.sharding import PartitionSpec as P

D = 8192
HEADS = 64
KVH = 8
HD = 128
DRAFT = 16
GROUP = HEADS // KVH
SCALING = 1.0 / math.sqrt(HD)
NEG = -1e30
LANES = 128
STREAMS = 1


def rope_tables(positions, head_size):
    steps_half = jnp.arange(head_size // 2).astype(jnp.float32)
    inverse = jnp.exp(steps_half * (-2.0 * math.log(500000.0) / head_size))
    angle = positions.astype(jnp.float32)[:, None] * inverse[None, :]
    return (jnp.cos(angle), jnp.sin(angle))


def rotate(values, cosine, sine_table):
    half = values.shape[-1] // 2
    first_half = values[..., :half]
    second_half = values[..., half:]
    cosine = cosine[:, None, :]
    sine_table = sine_table[:, None, :]
    return jnp.concatenate(
        [
            first_half * cosine - second_half * sine_table,
            second_half * cosine + first_half * sine_table,
        ],
        axis=-1,
    )


def rope_body(q_ref, k_ref, cos_ref, sin_ref, q_out, k_out):
    cosine = cos_ref[...]
    sine = sin_ref[...]
    for src, dst in ((q_ref, q_out), (k_ref, k_out)):
        for head in range(src.shape[1] // HD):
            cols = slice(head * HD, (head + 1) * HD)
            x = src[:, cols].astype(jnp.float32)
            turned = x * cosine + pltpu.roll(x, HD // 2, 1) * sine
            dst[:, cols] = turned.astype(jnp.bfloat16)


def rope(queries, keys, cosine, sine):
    return pl.pallas_call(
        rope_body,
        out_shape=(
            jax.ShapeDtypeStruct(queries.shape, jnp.bfloat16),
            jax.ShapeDtypeStruct(keys.shape, jnp.bfloat16),
        ),
        name="rope",
    )(queries, keys, cosine, sine)


def attend_body(meta, q_ref, k_ref, v_ref, *rest, seq0, draft):
    if draft:
        kn_ref, vn_ref, out_ref = rest
    else:
        (out_ref,) = rest
    valid = meta[1 + seq0 + pl.program_id(0)]
    kv_heads = k_ref.shape[2] // HD
    block = k_ref.shape[1]
    rows = GROUP * DRAFT
    lane = lax.broadcasted_iota(jnp.int32, (DRAFT, LANES), 1)
    usable = lax.broadcasted_iota(jnp.int32, (rows, block), 1) < valid
    stats = jnp.zeros((DRAFT, LANES), jnp.float32)
    nt = (((1,), (1,)), ((), ()))
    for kv in range(kv_heads):
        cols = slice(kv * HD, (kv + 1) * HD)
        heads = [kv * GROUP + g for g in range(GROUP)]
        q = jnp.concatenate([q_ref[:, h * HD : (h + 1) * HD] for h in heads], axis=0)
        s = lax.dot_general(q, k_ref[0, :, cols], nt, preferred_element_type=jnp.float32)
        s = jnp.where(usable, s * SCALING, NEG)
        peak = jnp.max(s, axis=1, keepdims=True)
        if draft:
            sd = lax.dot_general(q, kn_ref[:, cols], nt, preferred_element_type=jnp.float32)
            row = lax.broadcasted_iota(jnp.int32, sd.shape, 0) & (DRAFT - 1)
            causal = lax.broadcasted_iota(jnp.int32, sd.shape, 1) <= row
            sd = jnp.where(causal, sd * SCALING, NEG)
            peak = jnp.maximum(peak, jnp.max(sd, axis=1, keepdims=True))
        peak = peak.astype(jnp.bfloat16).astype(jnp.float32)
        w = jnp.where(usable, jnp.exp(s - peak), 0.0)
        den = jnp.sum(w, axis=1, keepdims=True)
        num = jnp.dot(w.astype(jnp.bfloat16), v_ref[0, :, cols], preferred_element_type=jnp.float32)
        if draft:
            wd = jnp.where(causal, jnp.exp(sd - peak), 0.0)
            den = den + jnp.sum(wd, axis=1, keepdims=True)
            num = num + jnp.dot(
                wd.astype(jnp.bfloat16), vn_ref[:, cols], preferred_element_type=jnp.float32
            )
        for g, h in enumerate(heads):
            part = slice(g * DRAFT, (g + 1) * DRAFT)
            out_ref[:, h * HD : (h + 1) * HD] = num[part].astype(jnp.bfloat16)
            stats = jnp.where(lane == h, den[part], stats)
            stats = jnp.where(lane == LANES // 2 + h, peak[part], stats)
    out_ref[:, -LANES:] = stats.astype(jnp.bfloat16)


def attend(meta, q, key_cache, value_cache, seq0, fresh=None):
    seqs = q.shape[0] // DRAFT
    width = q.shape[1]
    kv_width = width // GROUP
    block = key_cache.shape[1]
    cache_spec = pl.BlockSpec((1, block, kv_width), lambda s, meta: (seq0 + s, 0, meta[0]))
    in_specs = [pl.BlockSpec((DRAFT, width), lambda s, meta: (s, 0)), cache_spec, cache_spec]
    operands = [q, key_cache, value_cache]
    if fresh is not None:
        fresh_spec = pl.BlockSpec((DRAFT, kv_width), lambda s, meta: (s, 0))
        in_specs += [fresh_spec, fresh_spec]
        operands += list(fresh)
    return pl.pallas_call(
        functools.partial(attend_body, seq0=seq0, draft=fresh is not None),
        out_shape=jax.ShapeDtypeStruct((q.shape[0], width + LANES), jnp.bfloat16),
        grid_spec=pltpu.PrefetchScalarGridSpec(
            num_scalar_prefetch=1,
            grid=(seqs,),
            in_specs=in_specs,
            out_specs=pl.BlockSpec((DRAFT, width + LANES), lambda s, meta: (s, 0)),
        ),
        name="attend",
    )(meta, *operands)


def merge_body(*refs):
    *packs, out_ref = refs
    stats = [p[:, -LANES:].astype(jnp.float32) for p in packs]
    peaks = [pltpu.roll(s, LANES // 2, 1) for s in stats]
    top = functools.reduce(jnp.maximum, peaks)
    shares = [jnp.exp(p - top) for p in peaks]
    total = sum(w * s for w, s in zip(shares, stats))
    shares = [w / total for w in shares]
    for h in range(out_ref.shape[1] // HD):
        cols = slice(h * HD, (h + 1) * HD)
        acc = sum(w[:, h : h + 1] * p[:, cols].astype(jnp.float32) for w, p in zip(shares, packs))
        out_ref[:, cols] = acc.astype(jnp.bfloat16)


def merge(packs):
    rows, width = packs[0].shape
    return pl.pallas_call(
        merge_body,
        out_shape=jax.ShapeDtypeStruct((rows, width - LANES), jnp.bfloat16),
        name="merge",
    )(*packs)


def project_body(swap, *refs):
    n = len(refs) // 2 - 1
    parts, weight, outs, left = refs[:n], refs[n], refs[n + 1 : 2 * n + 1], refs[-1]
    rows = parts[0].shape[0]

    @pl.when(pl.program_id(0) == 0)
    def _():
        for t in range(n):
            start = pl.multiple_of((swap[0] ^ t) * rows, rows)
            left[pl.ds(start, rows), :] = parts[t][...]

    product = jnp.dot(left[...], weight[...], preferred_element_type=jnp.float32)
    for s in range(n):
        outs[s][...] = product[s * rows : (s + 1) * rows].astype(jnp.bfloat16)


def project(swap, parts, weight, tile):
    n = len(parts)
    rows, depth = parts[0].shape
    cols = weight.shape[1]
    return pl.pallas_call(
        project_body,
        out_shape=[jax.ShapeDtypeStruct((rows, cols), jnp.bfloat16)] * n,
        grid_spec=pltpu.PrefetchScalarGridSpec(
            num_scalar_prefetch=1,
            grid=(cols // tile,),
            in_specs=[pl.BlockSpec((rows, depth), lambda j, swap: (0, 0))] * n
            + [pl.BlockSpec((depth, tile), lambda j, swap: (0, j))],
            out_specs=[pl.BlockSpec((rows, tile), lambda j, swap: (0, j))] * n,
            scratch_shapes=[pltpu.VMEM((n * rows, depth), jnp.bfloat16)],
        ),
        name="project",
    )(swap, *parts, weight)


def gate_up_body(home, *refs, n, picks):
    parts, gain, gate_w, up_w = refs[:n], refs[n], refs[n + 1], refs[n + 2]
    outs = refs[n + 3 : n + 3 + len(picks)]
    left, gate_acc, up_acc = refs[n + 3 + len(picks) :]
    t = pl.program_id(0)
    k = pl.program_id(1)
    last = pl.num_programs(1) - 1
    rows = parts[0].shape[0]
    depth = gate_w.shape[0]
    units = gate_w.shape[1]

    @pl.when(jnp.logical_and(t == 0, k == 0))
    def _():
        scale = gain[...].astype(jnp.float32)
        for s in range(n):
            scaled = (parts[s][...].astype(jnp.float32) * scale).astype(jnp.bfloat16)
            for c in range(left.shape[0]):
                left[c, s * rows : (s + 1) * rows, :] = scaled[:, c * depth : (c + 1) * depth]

    x = left[k]
    gate = jnp.dot(x, gate_w[...], preferred_element_type=jnp.float32)
    up = jnp.dot(x, up_w[...], preferred_element_type=jnp.float32)

    @pl.when(k == 0)
    def _():
        gate_acc[...] = gate
        up_acc[...] = up

    @pl.when(jnp.logical_and(k > 0, k < last))
    def _():
        gate_acc[...] += gate
        up_acc[...] += up

    for i in range(len(picks)):

        @pl.when(jnp.logical_and(k == last, t == i))
        def _(i=i):
            outs[i][:, :units] = (gate_acc[...] + gate).astype(jnp.bfloat16)
            outs[i][:, units:] = (up_acc[...] + up).astype(jnp.bfloat16)


def gate_up(home, parts, gain, gate_weight, up_weight, picks, units, steps):
    n = len(parts)
    rows, width = parts[0].shape
    depth = width // steps
    weight_spec = pl.BlockSpec((depth, units), lambda t, k, home: (k, home[0] ^ (picks[0] + t)))
    return pl.pallas_call(
        functools.partial(gate_up_body, n=n, picks=picks),
        out_shape=[jax.ShapeDtypeStruct((n * rows, 2 * units), jnp.bfloat16)] * len(picks),
        grid_spec=pltpu.PrefetchScalarGridSpec(
            num_scalar_prefetch=1,
            grid=(len(picks), steps),
            in_specs=[pl.BlockSpec((rows, width), lambda t, k, home: (0, 0))] * n
            + [pl.BlockSpec((1, width), lambda t, k, home: (0, 0)), weight_spec, weight_spec],
            out_specs=[pl.BlockSpec((n * rows, 2 * units), lambda t, k, home: (0, 0))] * len(picks),
            scratch_shapes=[
                pltpu.VMEM((steps, n * rows, depth), jnp.bfloat16),
                pltpu.VMEM((n * rows, units), jnp.float32),
                pltpu.VMEM((n * rows, units), jnp.float32),
            ],
        ),
        name="gate_up",
    )(home, *parts, gain, gate_weight, up_weight)


def activate_body(own_ref, core_ref, far_ref, square_ref, out_ref, *, width):
    units = out_ref.shape[1]
    factor = lax.rsqrt(square_ref[...] / width + 1e-05)
    total = (
        own_ref[...].astype(jnp.float32)
        + core_ref[...].astype(jnp.float32)
        + far_ref[...].astype(jnp.float32)
    )
    gate = total[:, :units] * factor
    up = total[:, units:] * factor
    out_ref[...] = (gate / (1.0 + jnp.exp(-gate)) * up).astype(jnp.bfloat16)


def activate(own, core, far, squares, width):
    rows, both = own.shape
    return pl.pallas_call(
        functools.partial(activate_body, width=width),
        out_shape=jax.ShapeDtypeStruct((rows, both // 2), jnp.bfloat16),
        name="activate",
    )(own, core, far, squares)


def down_body(home, *refs, n, m):
    acts, weight, outs, acc = refs[:n], refs[n], refs[n + 1 : n + 1 + m], refs[-1]
    t = pl.program_id(0)
    rows = outs[0].shape[0]
    for i in range(n):

        @pl.when(t == i)
        def _(i=i):
            product = jnp.dot(acts[i][...], weight[...], preferred_element_type=jnp.float32)
            if i == 0:
                acc[...] = product
            elif i < n - 1:
                acc[...] += product
            else:
                total = acc[...] + product
                for s in range(m):
                    outs[s][...] = total[s * rows : (s + 1) * rows].astype(jnp.bfloat16)


def down(home, acts, weight, m):
    n = len(acts)
    rows, units = acts[0].shape
    cols = weight.shape[1]
    return pl.pallas_call(
        functools.partial(down_body, n=n, m=m),
        out_shape=[jax.ShapeDtypeStruct((rows // m, cols), jnp.bfloat16)] * m,
        grid_spec=pltpu.PrefetchScalarGridSpec(
            num_scalar_prefetch=1,
            grid=(n,),
            in_specs=[pl.BlockSpec((rows, units), lambda t, home: (0, 0))] * n
            + [pl.BlockSpec((units, cols), lambda t, home: (home[0] ^ t, 0))],
            out_specs=[pl.BlockSpec((rows // m, cols), lambda t, home: (0, 0))] * m,
            scratch_shapes=[pltpu.VMEM((rows, cols), jnp.float32)],
        ),
        name="down",
    )(home, *acts, weight)


def exchange(value, axis, mask):
    size = lax.axis_size(axis)
    return lax.ppermute(value, axis, [(i, i ^ mask) for i in range(size)])


def paired(
    residual_in,
    queries,
    new_keys,
    new_values,
    key_cache,
    value_cache,
    cache_lengths,
    norm_gain,
    out_weight,
    gate_weight,
    up_weight,
    down_weight,
):
    n_ffn = lax.axis_size("ffn")
    n_hidden = lax.axis_size("hidden")
    seq_count = cache_lengths.shape[0]
    block = key_cache.shape[1]
    ffn_index = lax.axis_index("ffn").astype(jnp.int32)
    hidden_index = lax.axis_index("hidden").astype(jnp.int32)
    home = hidden_index[None]
    swap = (hidden_index ^ ffn_index)[None]
    positions = (cache_lengths[:, None] + jnp.arange(DRAFT, dtype=jnp.int32)[None, :]).reshape(-1)
    cosine, sine = rope_tables(positions, HD)
    cosine = jnp.concatenate([cosine, cosine], axis=1)
    sine = jnp.concatenate([-sine, sine], axis=1)
    query_rot, key_rot = rope(queries, new_keys, cosine, sine)
    valid = cache_lengths - ffn_index * block
    metas = [jnp.concatenate([(ffn_index ^ s)[None], valid]) for s in range(n_ffn)]
    gain = norm_gain[None, :]
    units = gate_weight.shape[1] // n_hidden

    rows = residual_in.shape[0] // STREAMS
    outputs = []
    for stream in range(STREAMS):
        span = slice(stream * rows, (stream + 1) * rows)
        seq0 = stream * (seq_count // STREAMS)
        q = query_rot[span]
        others = range(1, n_ffn)
        arrived = {s: exchange(q, "ffn", s) for s in (2, 3, 1)}
        packs = [attend(metas[0], q, key_cache, value_cache, seq0, (key_rot[span], new_values[span]))]
        for s in (2, 1, 3):
            partial = attend(metas[s], arrived[s], key_cache, value_cache, seq0)
            packs.append(exchange(partial, "ffn", s))
        attended = merge(packs)
        near = exchange(attended, "hidden", 1)
        far = exchange(attended, "hidden", 2)
        far_near = exchange(far, "hidden", 1)
        shares = project(swap, [attended, near, far, far_near], out_weight, 512)
        received = [shares[0]] + [exchange(shares[s], "ffn", s) for s in others]
        projected = sum(r.astype(jnp.float32) for r in received)
        resid = (residual_in[span].astype(jnp.float32) + projected).astype(jnp.bfloat16)
        parts = [resid] + [exchange(resid, "ffn", s) for s in others]
        squares = jnp.concatenate(
            [jnp.sum(jnp.square(p.astype(jnp.float32)), axis=1, keepdims=True) for p in parts], axis=0
        )
        squares = squares + exchange(squares, "hidden", 1)
        squares = squares + exchange(squares, "hidden", 2)
        away, away_near = gate_up(home, parts, gain, gate_weight, up_weight, (2, 3), units, 4)
        crossing = (
            away.astype(jnp.float32) + exchange(away_near, "hidden", 1).astype(jnp.float32)
        ).astype(jnp.bfloat16)
        crossed = exchange(crossing, "hidden", 2)
        own, own_near = gate_up(home, parts, gain, gate_weight, up_weight, (0, 1), units, 4)
        act = activate(own, exchange(own_near, "hidden", 1), crossed, squares, D)
        act_far = exchange(act, "hidden", 2)
        acts = [act, exchange(act, "hidden", 1), act_far, exchange(act_far, "hidden", 1)]
        lowered = down(home, acts, down_weight, n_ffn)
        gathered = [lowered[0]] + [exchange(lowered[s], "ffn", s) for s in others]
        total = sum(g.astype(jnp.float32) for g in gathered)
        outputs.append((resid.astype(jnp.float32) + total).astype(jnp.bfloat16))
    return outputs[0] if STREAMS == 1 else jnp.concatenate(outputs, axis=0)


def shards(
    residual_in,
    queries,
    new_keys,
    new_values,
    key_cache,
    value_cache,
    cache_lengths,
    norm_gain,
    out_weight,
    gate_weight,
    up_weight,
    down_weight,
):
    group = HEADS // KVH
    seq_count = cache_lengths.shape[0]
    block = key_cache.shape[1]
    query_all, key_fresh, value_fresh = (
        lax.all_gather(queries, "ffn", axis=1, tiled=True),
        lax.all_gather(new_keys, "ffn", axis=1, tiled=True),
        lax.all_gather(new_values, "ffn", axis=1, tiled=True),
    )
    positions = (cache_lengths[:, None] + jnp.arange(DRAFT, dtype=jnp.int32)[None, :]).reshape(-1)
    cosine, sine_table = rope_tables(positions, HD)
    query_rot = rotate(
        query_all.astype(jnp.float32).reshape(-1, HEADS, HD), cosine, sine_table
    ).astype(jnp.bfloat16)
    query_rot = query_rot.reshape(seq_count, DRAFT, KVH, group, HD)
    key_rot = rotate(key_fresh.astype(jnp.float32).reshape(-1, KVH, HD), cosine, sine_table).astype(
        jnp.bfloat16
    )
    key_rot = key_rot.reshape(seq_count, DRAFT, KVH, HD)
    value_rows = value_fresh.reshape(seq_count, DRAFT, KVH, HD)
    cached_keys = key_cache.reshape(seq_count, block, KVH, HD)
    cached_values = value_cache.reshape(seq_count, block, KVH, HD)
    scaling = 1.0 / math.sqrt(HD)
    cache_scores = (
        jnp.einsum("sjkgd,spkd->sjkgp", query_rot, cached_keys, preferred_element_type=jnp.float32)
        * scaling
    )
    draft_scores = (
        jnp.einsum("sjkgd,sikd->sjkgi", query_rot, key_rot, preferred_element_type=jnp.float32)
        * scaling
    )
    ffn_index = lax.axis_index("ffn")
    slot_positions = ffn_index * block + jnp.arange(block, dtype=jnp.int32)
    usable = (slot_positions[None, :] < cache_lengths[:, None])[:, None, None, None, :]
    causal = jnp.arange(DRAFT)[None, :] <= jnp.arange(DRAFT)[:, None]
    draft_usable = jnp.logical_and(causal[None, :, None, None, :], ffn_index == 0)
    cache_scores = jnp.where(usable, cache_scores, -1e30)
    draft_scores = jnp.where(draft_usable, draft_scores, -1e30)
    local_peak = jnp.maximum(cache_scores.max(-1), draft_scores.max(-1))
    peak_score = lax.pmax(local_peak, "ffn")[..., None]
    cache_weights = jnp.where(usable, jnp.exp(cache_scores - peak_score), 0.0)
    draft_weights = jnp.where(draft_usable, jnp.exp(draft_scores - peak_score), 0.0)
    numerator = jnp.einsum(
        "sjkgp,spkd->sjkgd",
        cache_weights.astype(jnp.bfloat16),
        cached_values,
        preferred_element_type=jnp.float32,
    )
    numerator = numerator + jnp.einsum(
        "sjkgi,sikd->sjkgd",
        draft_weights.astype(jnp.bfloat16),
        value_rows,
        preferred_element_type=jnp.float32,
    )
    denominator = cache_weights.sum(-1) + draft_weights.sum(-1)
    row_count = seq_count * DRAFT
    numerator = numerator.reshape(row_count, HEADS, HD)
    denominator = denominator.reshape(row_count, HEADS)
    heads_here = out_weight.shape[0] // HD
    numerator_share, denominator_share = (
        lax.psum_scatter(
            numerator.astype(jnp.bfloat16), "ffn", scatter_dimension=1, tiled=True
        ).astype(jnp.float32),
        lax.psum_scatter(
            denominator.astype(jnp.bfloat16), "ffn", scatter_dimension=1, tiled=True
        ).astype(jnp.float32),
    )
    attended = (
        (numerator_share / denominator_share[..., None])
        .reshape(row_count, heads_here * HD)
        .astype(jnp.bfloat16)
    )
    attended_rows = lax.all_gather(attended, "hidden", axis=0, tiled=True)
    projected = lax.psum_scatter(
        jnp.dot(attended_rows, out_weight, preferred_element_type=jnp.float32).astype(jnp.bfloat16),
        "ffn",
        scatter_dimension=0,
        tiled=True,
    ).astype(jnp.float32)
    resid = (residual_in.astype(jnp.float32) + projected).astype(jnp.bfloat16)
    widened = resid.astype(jnp.float32)
    squares = lax.psum(jnp.sum(widened * widened, axis=1), "hidden")
    factor = lax.rsqrt(squares / D + 1e-05)[:, None]
    normed = (widened * factor * norm_gain.astype(jnp.float32)[None, :]).astype(jnp.bfloat16)
    units_here = gate_weight.shape[1]
    piece = lax.all_gather(normed, "ffn", axis=0, tiled=True)
    partial_inner = jnp.concatenate(
        [
            jnp.dot(piece, gate_weight, preferred_element_type=jnp.float32),
            jnp.dot(piece, up_weight, preferred_element_type=jnp.float32),
        ],
        axis=1,
    )
    summed = lax.psum(partial_inner.astype(jnp.bfloat16), "hidden").astype(jnp.float32)
    activation = (jax.nn.silu(summed[:, :units_here]) * summed[:, units_here:]).astype(jnp.bfloat16)
    lowered = lax.psum_scatter(
        jnp.dot(activation, down_weight, preferred_element_type=jnp.float32).astype(jnp.bfloat16),
        "ffn",
        scatter_dimension=0,
        tiled=True,
    ).astype(jnp.float32)
    return (widened + lowered).astype(jnp.bfloat16)


def solution(mesh):
    in_specs = (
        P(("groups", "ffn"), "hidden"),
        P(("groups", "hidden"), "ffn"),
        P(("groups", "hidden"), "ffn"),
        P(("groups", "hidden"), "ffn"),
        P(("groups", "hidden"), "ffn", None),
        P(("groups", "hidden"), "ffn", None),
        P(("groups", "hidden")),
        P("hidden"),
        P("ffn", "hidden"),
        P("hidden", "ffn"),
        P("hidden", "ffn"),
        P("ffn", "hidden"),
    )
    out_specs = P(("groups", "ffn"), "hidden")
    four = mesh.shape["ffn"] == 4 and mesh.shape["hidden"] == 4
    return jax.shard_map(paired if four else shards, mesh=mesh, in_specs=in_specs, out_specs=out_specs, check_vma=False)
```

```python
import functools
import math

import jax
import jax.numpy as jnp
from jax import lax
from jax.experimental import pallas as pl
from jax.experimental.pallas import tpu as pltpu
from jax.sharding import PartitionSpec as P

D = 8192
HEADS = 64
KVH = 8
HD = 128
DRAFT = 16
GROUP = HEADS // KVH
SCALING = 1.0 / math.sqrt(HD)
NEG = -1e30
LOW = -1e28
LANES = 128
STREAMS = 1
COST = 1
SLOTS = (2, 3, 1)
HOME, SWAP, NOWHERE = 1, 2, 3


def rope_tables(positions, head_size):
    steps_half = jnp.arange(head_size // 2).astype(jnp.float32)
    inverse = jnp.exp(steps_half * (-2.0 * math.log(500000.0) / head_size))
    angle = positions.astype(jnp.float32)[:, None] * inverse[None, :]
    return (jnp.cos(angle), jnp.sin(angle))


def rotate(values, cosine, sine_table):
    half = values.shape[-1] // 2
    first_half = values[..., :half]
    second_half = values[..., half:]
    cosine = cosine[:, None, :]
    sine_table = sine_table[:, None, :]
    return jnp.concatenate(
        [
            first_half * cosine - second_half * sine_table,
            second_half * cosine + first_half * sine_table,
        ],
        axis=-1,
    )


SMEM_SPEC = pl.BlockSpec(memory_space=pltpu.SMEM)
VMEM_SPEC = pl.BlockSpec(memory_space=pltpu.VMEM)
ANY_SPEC = pl.BlockSpec(memory_space=pl.ANY)
NT = (((1,), (1,)), ((), ()))


def bf16(*shape):
    return jax.ShapeDtypeStruct(shape, jnp.bfloat16)


class Chain:
    def __init__(self):
        self.token = None

    def __call__(self, name, body, operands, outs, scratch=(), mib=4, flops=1, in_vmem=False):
        before = () if self.token is None else (self.token,)
        skip = len(before)
        n_in = len(operands)
        n_out = len(outs)

        def run(*refs):
            ins = refs[skip : skip + n_in]
            body(ins, refs[skip + n_in : skip + n_in + n_out], refs[skip + n_in + n_out + 1 :])

        shapes = [pltpu.VMEM(o.shape, o.dtype) if in_vmem else o for o in outs]
        *results, self.token = pl.pallas_call(
            run,
            out_shape=shapes + [jax.ShapeDtypeStruct((8, LANES), jnp.float32)],
            in_specs=[ANY_SPEC] * skip + [spec for _, spec in operands],
            out_specs=[VMEM_SPEC] * n_out + [ANY_SPEC],
            scratch_shapes=list(scratch),
            compiler_params=pltpu.CompilerParams(vmem_limit_bytes=mib * 1024 * 1024),
            cost_estimate=pl.CostEstimate(
                flops=flops * COST, transcendentals=0, bytes_accessed=1 << 20
            ),
            name=name,
        )(*before, *[value for value, _ in operands])
        return results


def rope_body(ins, outs, scratch, *, pieces):
    q_ref, k_ref, cos_ref, sin_ref = ins[:4]
    cosine = cos_ref[...]
    sine = sin_ref[...]
    rows = cosine.shape[0] // pieces
    for src, dsts in ((q_ref, outs[:pieces]), (k_ref, outs[pieces:])):
        for head in range(src.shape[1] // HD):
            cols = slice(head * HD, (head + 1) * HD)
            x = src[:, cols].astype(jnp.float32)
            turned = (x * cosine + pltpu.roll(x, HD // 2, 1) * sine).astype(jnp.bfloat16)
            for i, dst in enumerate(dsts):
                dst[:, cols] = turned[i * rows : (i + 1) * rows]


def load_body(ins, outs, scratch, *, plan, place):
    at, *sources = ins
    (sems,) = scratch
    copies = []
    for i, (which, mask, dim) in enumerate(plan):
        size = outs[i].shape[dim]
        start = pl.multiple_of((at[place] ^ mask) * size, LANES)
        window = (slice(None), pl.ds(start, size)) if dim else (pl.ds(start, size), slice(None))
        copy = pltpu.make_async_copy(sources[which].at[window], outs[i], sems.at[i])
        copy.start()
        copies.append(copy)
    for copy in copies:
        copy.wait()


def attend_body(ins, outs, scratch, *, seq0, slot):
    draft = slot == 0
    at_ref, len_ref, q_ref, k_hbm, v_hbm, *fresh = ins
    (out_ref,) = outs
    k_buf, v_buf, sems = scratch
    seqs, block, kv_width = k_buf.shape
    start = pl.multiple_of((at_ref[0] ^ slot) * kv_width, LANES)
    copies = []
    for s in range(seqs):
        pair = []
        for i, (src, dst) in enumerate(((k_hbm, k_buf), (v_hbm, v_buf))):
            copy = pltpu.make_async_copy(
                src.at[seq0 + s, :, pl.ds(start, kv_width)], dst.at[s], sems.at[i, s]
            )
            copy.start()
            pair.append(copy)
        copies.append(pair)
    lane = lax.broadcasted_iota(jnp.int32, (DRAFT, LANES), 1)
    position = lax.broadcasted_iota(jnp.int32, (GROUP * DRAFT, block), 1)
    for s in range(seqs):
        for copy in copies[s]:
            copy.wait()
        span = slice(s * DRAFT, (s + 1) * DRAFT)
        usable = position < len_ref[seq0 + s] - at_ref[0] * block
        stats = jnp.zeros((DRAFT, LANES), jnp.float32)
        for kv in range(kv_width // HD):
            cols = slice(kv * HD, (kv + 1) * HD)
            heads = [kv * GROUP + g for g in range(GROUP)]
            q = jnp.concatenate([q_ref[span, h * HD : (h + 1) * HD] for h in heads], axis=0)
            raw = lax.dot_general(q, k_buf[s, :, cols], NT, preferred_element_type=jnp.float32)
            raw = jnp.where(usable, raw, NEG)
            peak = jnp.max(raw, axis=1, keepdims=True)
            if draft:
                raw_d = lax.dot_general(
                    q, fresh[0][span, cols], NT, preferred_element_type=jnp.float32
                )
                row = lax.broadcasted_iota(jnp.int32, raw_d.shape, 0) & (DRAFT - 1)
                causal = lax.broadcasted_iota(jnp.int32, raw_d.shape, 1) <= row
                raw_d = jnp.where(causal, raw_d, NEG)
                peak = jnp.maximum(peak, jnp.max(raw_d, axis=1, keepdims=True))
            peak = jnp.maximum(peak * SCALING, LOW).astype(jnp.bfloat16).astype(jnp.float32)
            w = jnp.exp(raw * SCALING - peak)
            den = jnp.sum(w, axis=1, keepdims=True)
            num = jnp.dot(
                w.astype(jnp.bfloat16), v_buf[s, :, cols], preferred_element_type=jnp.float32
            )
            if draft:
                w_d = jnp.exp(raw_d * SCALING - peak)
                den = den + jnp.sum(w_d, axis=1, keepdims=True)
                num = num + jnp.dot(
                    w_d.astype(jnp.bfloat16),
                    fresh[1][span, cols],
                    preferred_element_type=jnp.float32,
                )
            for g, h in enumerate(heads):
                part = slice(g * DRAFT, (g + 1) * DRAFT)
                out_ref[span, h * HD : (h + 1) * HD] = num[part].astype(jnp.bfloat16)
                stats = jnp.where(lane == h, den[part], stats)
                stats = jnp.where(lane == LANES // 2 + h, peak[part], stats)
        out_ref[span, -LANES:] = stats.astype(jnp.bfloat16)


def merge_body(packs, outs, scratch):
    (out_ref,) = outs
    stats = [p[:, -LANES:].astype(jnp.float32) for p in packs]
    peaks = [pltpu.roll(s, LANES // 2, 1) for s in stats]
    top = functools.reduce(jnp.maximum, peaks)
    shares = [jnp.exp(p - top) for p in peaks]
    total = sum(w * s for w, s in zip(shares, stats))
    shares = [w / total for w in shares]
    for h in range(out_ref.shape[1] // HD):
        cols = slice(h * HD, (h + 1) * HD)
        acc = sum(w[:, h : h + 1] * p[:, cols].astype(jnp.float32) for w, p in zip(shares, packs))
        out_ref[:, cols] = acc.astype(jnp.bfloat16)


def project_body(ins, outs, scratch, *, tile):
    places, *parts, weight = ins
    (left,) = scratch
    rows = parts[0].shape[0]
    for t, part in enumerate(parts):
        start = pl.multiple_of((places[SWAP] ^ t) * rows, rows)
        left[pl.ds(start, rows), :] = part[...]
    for lo in range(0, weight.shape[1], tile):
        cols = slice(lo, lo + tile)
        product = jnp.dot(left[...], weight[:, cols], preferred_element_type=jnp.float32)
        for s, out in enumerate(outs):
            out[:, cols] = product[s * rows : (s + 1) * rows].astype(jnp.bfloat16)


def resid_body(ins, outs, scratch):
    base, *shares = ins
    projected = sum(s[...].astype(jnp.float32) for s in shares)
    outs[0][...] = (base[...].astype(jnp.float32) + projected).astype(jnp.bfloat16)


def prepare_body(ins, outs, scratch):
    *parts, gain = ins
    left, squares = outs
    rows, width = parts[0].shape
    scale = gain[...].astype(jnp.float32)
    for s, part in enumerate(parts):
        left[s * rows : (s + 1) * rows, :] = (part[...].astype(jnp.float32) * scale).astype(
            jnp.bfloat16
        )
    wide = jnp.concatenate([p[...].astype(jnp.float32) for p in parts], axis=0)
    squares[...] = lax.dot_general(
        jnp.ones((8, width), jnp.float32),
        wide * wide,
        NT,
        preferred_element_type=jnp.float32,
        precision=lax.Precision.HIGHEST,
    )


def gate_up_body(ins, outs, scratch):
    left, *weights = ins
    (out,) = outs
    units = weights[0].shape[1]
    for m, weight in enumerate(weights):
        product = jnp.dot(left[...], weight[...], preferred_element_type=jnp.float32)
        out[:, m * units : (m + 1) * units] = product.astype(jnp.bfloat16)


def add_body(ins, outs, scratch):
    outs[0][...] = (ins[0][...].astype(jnp.float32) + ins[1][...].astype(jnp.float32)).astype(
        jnp.bfloat16
    )


def activate_body(ins, outs, scratch, *, width):
    own_ref, core_ref, far_ref, *square_refs = ins
    (out_ref,) = outs
    units = out_ref.shape[1]
    pick = (lax.broadcasted_iota(jnp.int32, (8, LANES), 0) == 0).astype(jnp.float32)
    squares = lax.dot_general(
        sum(r[...] for r in square_refs),
        pick,
        (((0,), (0,)), ((), ())),
        preferred_element_type=jnp.float32,
        precision=lax.Precision.HIGHEST,
    )
    factor = lax.rsqrt(squares[:, :1] / width + 1e-05)
    total = (
        own_ref[...].astype(jnp.float32)
        + core_ref[...].astype(jnp.float32)
        + far_ref[...].astype(jnp.float32)
    )
    gate = total[:, :units] * factor
    up = total[:, units:] * factor
    out_ref[...] = (gate / (1.0 + jnp.exp(-gate)) * up).astype(jnp.bfloat16)


def down_body(ins, outs, scratch, *, tile):
    acts, weights = ins[: len(ins) // 2], ins[len(ins) // 2 :]
    rows = outs[0].shape[0]
    for lo in range(0, weights[0].shape[1], tile):
        cols = slice(lo, lo + tile)
        product = sum(
            jnp.dot(a[...], w[:, cols], preferred_element_type=jnp.float32)
            for a, w in zip(acts, weights)
        )
        for s, out in enumerate(outs):
            out[:, cols] = product[s * rows : (s + 1) * rows].astype(jnp.bfloat16)


def exchange(value, axis, mask):
    size = lax.axis_size(axis)
    return lax.ppermute(value, axis, [(i, i ^ mask) for i in range(size)])


def paired(
    residual_in,
    queries,
    new_keys,
    new_values,
    key_cache,
    value_cache,
    cache_lengths,
    norm_gain,
    out_weight,
    gate_weight,
    up_weight,
    down_weight,
):
    n_ffn = lax.axis_size("ffn")
    n_hidden = lax.axis_size("hidden")
    seq_count = cache_lengths.shape[0]
    block = key_cache.shape[1]
    ffn_index = lax.axis_index("ffn").astype(jnp.int32)
    hidden_index = lax.axis_index("hidden").astype(jnp.int32)
    in_hbm = pltpu.with_memory_space_constraint
    places = jnp.stack([ffn_index, hidden_index, hidden_index ^ ffn_index, jnp.zeros((), jnp.int32)])
    at = (places, SMEM_SPEC)
    lengths = (in_hbm(cache_lengths, pltpu.HBM), SMEM_SPEC)
    gain = norm_gain[None, :]

    positions = (cache_lengths[:, None] + jnp.arange(DRAFT, dtype=jnp.int32)[None, :]).reshape(-1)
    half = HD // 2
    lanes = jnp.arange(HD)
    inverse = jnp.exp((lanes % half).astype(jnp.float32) * (-2.0 * math.log(500000.0) / HD))
    angle = positions.astype(jnp.float32)[:, None] * inverse[None, :]
    cosine = jnp.cos(angle)
    sine = jnp.where(lanes < half, -1.0, 1.0)[None, :] * jnp.sin(angle)

    chain = Chain()
    vm = lambda *values: [(v, VMEM_SPEC) for v in values]
    hbm = lambda *values: [(in_hbm(v, pltpu.HBM), ANY_SPEC) for v in values]
    n = n_ffn
    total_rows, width = residual_in.shape
    rows = total_rows // STREAMS
    seqs = seq_count // STREAMS
    q_width = queries.shape[1]
    kv_width = new_keys.shape[1]
    units = gate_weight.shape[1] // n_hidden
    streams = range(STREAMS)
    spans = [slice(i * rows, (i + 1) * rows) for i in streams]

    rotated = chain(
        "rope",
        functools.partial(rope_body, pieces=STREAMS),
        vm(queries, new_keys, cosine, sine) + [(places, ANY_SPEC), (gain, ANY_SPEC)],
        [bf16(rows, q_width)] * STREAMS + [bf16(rows, kv_width)] * STREAMS,
    )
    q, k_new = rotated[:STREAMS], rotated[STREAMS:]
    arrived = [{s: exchange(q[i], "ffn", s) for s in SLOTS} for i in streams]

    def attend(i, slot):
        cache = pltpu.VMEM((seqs, block, kv_width), jnp.bfloat16)
        operands = [at, lengths] + vm(q[i] if slot == 0 else arrived[i][slot])
        operands += hbm(key_cache, value_cache)
        if slot == 0:
            operands += vm(k_new[i]) + [(in_hbm(new_values[spans[i]], pltpu.HBM), VMEM_SPEC)]
        (packed,) = chain(
            "attend",
            functools.partial(attend_body, seq0=i * seqs, slot=slot),
            operands,
            [bf16(rows, q_width + LANES)],
            [cache, cache, pltpu.SemaphoreType.DMA((2, seqs))],
            mib=6,
            flops=4,
        )
        return packed if slot == 0 else exchange(packed, "ffn", slot)

    def load(place, sources, plan, outs):
        return chain(
            "load",
            functools.partial(load_body, plan=plan, place=place),
            [at] + hbm(*sources),
            outs,
            [pltpu.SemaphoreType.DMA((len(outs),))],
            flops=4,
            in_vmem=True,
        )

    def load_units(t):
        plan = [(0, t, 1), (1, t, 1)]
        return load(HOME, (gate_weight, up_weight), plan, [bf16(width, units)] * 2)

    packs = [[attend(i, 0)] for i in streams]
    (out_w,) = load(NOWHERE, (out_weight,), [(0, 0, 0)], [bf16(*out_weight.shape)])
    unit_w = {3: load_units(3)}
    for i in streams:
        for s in SLOTS:
            packs[i].append(attend(i, s))
            if 2 not in unit_w:
                unit_w[2] = load_units(2)
    unit_w.update({t: load_units(t) for t in (1, 0)})
    down_plan = [(0, t, 0) for t in range(n_hidden)]
    down_w = load(HOME, (down_weight,), down_plan, [bf16(units, width)] * n_hidden)

    shares = []
    for i in streams:
        (attended,) = chain("merge", merge_body, vm(*packs[i]), [bf16(rows, q_width)], flops=1)
        near = exchange(attended, "hidden", 1)
        far = exchange(attended, "hidden", 2)
        far_near = exchange(far, "hidden", 1)
        out = chain(
            "project",
            functools.partial(project_body, tile=512),
            [at] + vm(attended, near, far, far_near, out_w),
            [bf16(rows, width)] * n,
            [pltpu.VMEM((n * rows, q_width), jnp.bfloat16)],
            flops=3,
        )
        shares.append([out[0]] + [exchange(out[s], "ffn", s) for s in range(1, n)])

    resid, parts = [], []
    for i in streams:
        (r,) = chain("resid", resid_body, vm(residual_in[spans[i]], *shares[i]), [bf16(rows, width)])
        resid.append(r)
        parts.append([r] + [exchange(r, "ffn", s) for s in range(1, n)])

    owns, sums = [], []
    for i in streams:
        left, squares = chain(
            "prepare",
            prepare_body,
            vm(*parts[i], gain),
            [bf16(n * rows, width), jax.ShapeDtypeStruct((8, n * rows), jnp.float32)],
            mib=8,
        )

        away_squares = [exchange(squares, "hidden", t) for t in range(1, n_hidden)]

        def gate_up(t):
            (product,) = chain(
                "gate_up", gate_up_body, vm(left, *unit_w[t]), [bf16(n * rows, 2 * units)], flops=3
            )
            return product

        away_near = exchange(gate_up(3), "hidden", 1)
        away = gate_up(2)
        (crossing,) = chain("add", add_body, vm(away, away_near), [bf16(n * rows, 2 * units)])
        crossed = exchange(crossing, "hidden", 2)
        own_near = exchange(gate_up(1), "hidden", 1)
        own = gate_up(0)
        sums.append((own, own_near, crossed, squares, *away_squares))

    acts = []
    for i in streams:
        (act,) = chain(
            "activate",
            functools.partial(activate_body, width=D),
            vm(*sums[i]),
            [bf16(n * rows, units)],
            mib=8,
        )
        far = exchange(act, "hidden", 2)
        acts.append([act, exchange(act, "hidden", 1), far, exchange(far, "hidden", 1)])

    lowered = []
    for i in streams:
        out = chain(
            "down",
            functools.partial(down_body, tile=512),
            vm(*acts[i], *down_w),
            [bf16(rows, width)] * n,
            flops=5,
        )
        lowered.append([out[0]] + [exchange(out[s], "ffn", s) for s in range(1, n)])

    finals = [
        chain("final", resid_body, vm(resid[i], *lowered[i]), [bf16(rows, width)])[0]
        for i in streams
    ]
    return finals[0] if STREAMS == 1 else jnp.concatenate(finals, axis=0)


def shards(
    residual_in,
    queries,
    new_keys,
    new_values,
    key_cache,
    value_cache,
    cache_lengths,
    norm_gain,
    out_weight,
    gate_weight,
    up_weight,
    down_weight,
):
    group = HEADS // KVH
    seq_count = cache_lengths.shape[0]
    block = key_cache.shape[1]
    query_all, key_fresh, value_fresh = (
        lax.all_gather(queries, "ffn", axis=1, tiled=True),
        lax.all_gather(new_keys, "ffn", axis=1, tiled=True),
        lax.all_gather(new_values, "ffn", axis=1, tiled=True),
    )
    positions = (cache_lengths[:, None] + jnp.arange(DRAFT, dtype=jnp.int32)[None, :]).reshape(-1)
    cosine, sine_table = rope_tables(positions, HD)
    query_rot = rotate(
        query_all.astype(jnp.float32).reshape(-1, HEADS, HD), cosine, sine_table
    ).astype(jnp.bfloat16)
    query_rot = query_rot.reshape(seq_count, DRAFT, KVH, group, HD)
    key_rot = rotate(key_fresh.astype(jnp.float32).reshape(-1, KVH, HD), cosine, sine_table).astype(
        jnp.bfloat16
    )
    key_rot = key_rot.reshape(seq_count, DRAFT, KVH, HD)
    value_rows = value_fresh.reshape(seq_count, DRAFT, KVH, HD)
    cached_keys = key_cache.reshape(seq_count, block, KVH, HD)
    cached_values = value_cache.reshape(seq_count, block, KVH, HD)
    scaling = 1.0 / math.sqrt(HD)
    cache_scores = (
        jnp.einsum("sjkgd,spkd->sjkgp", query_rot, cached_keys, preferred_element_type=jnp.float32)
        * scaling
    )
    draft_scores = (
        jnp.einsum("sjkgd,sikd->sjkgi", query_rot, key_rot, preferred_element_type=jnp.float32)
        * scaling
    )
    ffn_index = lax.axis_index("ffn")
    slot_positions = ffn_index * block + jnp.arange(block, dtype=jnp.int32)
    usable = (slot_positions[None, :] < cache_lengths[:, None])[:, None, None, None, :]
    causal = jnp.arange(DRAFT)[None, :] <= jnp.arange(DRAFT)[:, None]
    draft_usable = jnp.logical_and(causal[None, :, None, None, :], ffn_index == 0)
    cache_scores = jnp.where(usable, cache_scores, -1e30)
    draft_scores = jnp.where(draft_usable, draft_scores, -1e30)
    local_peak = jnp.maximum(cache_scores.max(-1), draft_scores.max(-1))
    peak_score = lax.pmax(local_peak, "ffn")[..., None]
    cache_weights = jnp.where(usable, jnp.exp(cache_scores - peak_score), 0.0)
    draft_weights = jnp.where(draft_usable, jnp.exp(draft_scores - peak_score), 0.0)
    numerator = jnp.einsum(
        "sjkgp,spkd->sjkgd",
        cache_weights.astype(jnp.bfloat16),
        cached_values,
        preferred_element_type=jnp.float32,
    )
    numerator = numerator + jnp.einsum(
        "sjkgi,sikd->sjkgd",
        draft_weights.astype(jnp.bfloat16),
        value_rows,
        preferred_element_type=jnp.float32,
    )
    denominator = cache_weights.sum(-1) + draft_weights.sum(-1)
    row_count = seq_count * DRAFT
    numerator = numerator.reshape(row_count, HEADS, HD)
    denominator = denominator.reshape(row_count, HEADS)
    heads_here = out_weight.shape[0] // HD
    numerator_share, denominator_share = (
        lax.psum_scatter(
            numerator.astype(jnp.bfloat16), "ffn", scatter_dimension=1, tiled=True
        ).astype(jnp.float32),
        lax.psum_scatter(
            denominator.astype(jnp.bfloat16), "ffn", scatter_dimension=1, tiled=True
        ).astype(jnp.float32),
    )
    attended = (
        (numerator_share / denominator_share[..., None])
        .reshape(row_count, heads_here * HD)
        .astype(jnp.bfloat16)
    )
    attended_rows = lax.all_gather(attended, "hidden", axis=0, tiled=True)
    projected = lax.psum_scatter(
        jnp.dot(attended_rows, out_weight, preferred_element_type=jnp.float32).astype(jnp.bfloat16),
        "ffn",
        scatter_dimension=0,
        tiled=True,
    ).astype(jnp.float32)
    resid = (residual_in.astype(jnp.float32) + projected).astype(jnp.bfloat16)
    widened = resid.astype(jnp.float32)
    squares = lax.psum(jnp.sum(widened * widened, axis=1), "hidden")
    factor = lax.rsqrt(squares / D + 1e-05)[:, None]
    normed = (widened * factor * norm_gain.astype(jnp.float32)[None, :]).astype(jnp.bfloat16)
    units_here = gate_weight.shape[1]
    piece = lax.all_gather(normed, "ffn", axis=0, tiled=True)
    partial_inner = jnp.concatenate(
        [
            jnp.dot(piece, gate_weight, preferred_element_type=jnp.float32),
            jnp.dot(piece, up_weight, preferred_element_type=jnp.float32),
        ],
        axis=1,
    )
    summed = lax.psum(partial_inner.astype(jnp.bfloat16), "hidden").astype(jnp.float32)
    activation = (jax.nn.silu(summed[:, :units_here]) * summed[:, units_here:]).astype(jnp.bfloat16)
    lowered = lax.psum_scatter(
        jnp.dot(activation, down_weight, preferred_element_type=jnp.float32).astype(jnp.bfloat16),
        "ffn",
        scatter_dimension=0,
        tiled=True,
    ).astype(jnp.float32)
    return (widened + lowered).astype(jnp.bfloat16)


def solution(mesh):
    in_specs = (
        P(("groups", "ffn"), "hidden"),
        P(("groups", "hidden"), "ffn"),
        P(("groups", "hidden"), "ffn"),
        P(("groups", "hidden"), "ffn"),
        P(("groups", "hidden"), "ffn", None),
        P(("groups", "hidden"), "ffn", None),
        P(("groups", "hidden")),
        P("hidden"),
        P("ffn", "hidden"),
        P("hidden", "ffn"),
        P("hidden", "ffn"),
        P("ffn", "hidden"),
    )
    out_specs = P(("groups", "ffn"), "hidden")
    four = mesh.shape["ffn"] == 4 and mesh.shape["hidden"] == 4
    return jax.shard_map(paired if four else shards, mesh=mesh, in_specs=in_specs, out_specs=out_specs, check_vma=False)
```
